32 devices in a mesh: region: 8 (over z, x), tm: 4 (over y, core).
Axes of the slice: x: 2, y: 2, z: 4, core: 2. Of those that a mesh axis runs over, the one named last changes fastest.
Arguments:
- observations: bfloat16 [8, 4, 2048, 512], P('region', 'tm'), may hold values from -160 to 160
- counts: int32 [8, 4], P('region', 'tm'), may hold values from 1 to 8, as said below
- visible: int32 [8, 8], replicated, may hold values 0 or 1
- latents: bfloat16 [8, 32, 512], P('region'), may hold values from -6 to 6
- lat_gain: float32 [512], replicated, may hold values from 0.5 to 1.5
- mlp_gain: float32 [512], replicated, may hold values from 0.5 to 1.5
- w_query: bfloat16 [512, 512], replicated, may hold values from -0.25 to 0.25
- w_keyval: bfloat16 [512, 1024], replicated, may hold values from -0.25 to 0.25
- w_out: bfloat16 [512, 512], replicated, may hold values from -0.25 to 0.25
- w_up: bfloat16 [512, 2048], P(None, 'tm'), may hold values from -0.25 to 0.25
- w_down: bfloat16 [2048, 512], P('tm'), may hold values from -0.125 to 0.125
Outputs:
- encoded: bfloat16 [8, 32, 512], P('region')
The draws below stay inside these ranges and needn't reach their ends.
Inputs may be any that keep to these rules, and one draw needn't show every extreme that they name: `counts`: some region and time slot holds 8 blocks.
All inputs are finite; a program needn't handle non-finite values.
Results may differ from the reference program's by a relative error of at most 0.0055.
The reference program's roundings to bfloat16 on the way (of `keyval`, `normed`, `queries`, `attended`, `normed2` and `hidden`) count: a program that leaves them out, or rounds other values in their place, can miss the bound.
Values may be sent and summed in bfloat16 or wider, within the bound.
A program may use at most 64 MiB of HBM per device.

```python
import jax
import jax.numpy as jnp
from jax import lax

D = 512
H = 8
HID = 2048
DH = 64
LR = 32
CAP = 8
BLK = 256
REGIONS = 8
SLOTS = 4


def block_counts(key):
    heavy = jax.random.randint(jax.random.fold_in(key, 101), (REGIONS, 1), 0, 4) == 0
    upper = jax.random.randint(jax.random.fold_in(key, 102), (REGIONS, SLOTS), CAP // 2 + 1, CAP + 1)
    blocks = jnp.where(heavy, upper, 1).astype(jnp.int32).reshape(REGIONS * SLOTS)
    chosen = jax.random.randint(jax.random.fold_in(key, 103), (), 0, REGIONS * SLOTS)
    blocks = jnp.where(jnp.arange(REGIONS * SLOTS, dtype=jnp.int32) == chosen, CAP, blocks)
    return blocks.reshape(REGIONS, SLOTS).astype(jnp.int32)


def draw_counts(key, part):
    return block_counts(key)


def draw_observations(key, part):
    shape = (REGIONS, SLOTS, CAP * BLK, D)
    base_key = jax.random.fold_in(key, 201)
    values = jnp.clip(3.0 * jax.random.normal(base_key, shape, jnp.float32), -18.0, 18.0)
    return values.astype(jnp.bfloat16)


def touch_ends(entries, rng, smallest, high):
    longest = entries.shape.index(max(entries.shape))
    spots = []
    for shift in (0, 1):
        where = [jax.random.randint(jax.random.fold_in(rng, axis), (), 0, length) for axis, length in enumerate(entries.shape)]
        where[longest] = (where[longest] + shift) % entries.shape[longest]
        spots.append(tuple(where))
    return entries.at[spots[0]].set(smallest).at[spots[1]].set(high)


def levels(key, shape, cuts, least, top_value):
    def one(axis_at, shards_of):
        steps = jax.random.uniform(jax.random.fold_in(jax.random.fold_in(key, 6), axis_at), (shards_of,), jnp.float32, least / len(cuts), top_value / len(cuts))
        return jnp.repeat(jnp.exp(steps), shape[axis_at] // shards_of).reshape((-1,) + (1,) * (len(shape) - axis_at - 1))

    factor_of = one(*cuts[0])
    for cut in cuts[1:]:
        factor_of = factor_of * one(*cut)
    return factor_of


def gaussian(stream_key, dims, spread, bound, cuts=(), kind=jnp.bfloat16):
    drawn = jax.random.normal(stream_key, dims, jnp.float32) * spread
    if len(cuts) > 0:
        drawn = levels(stream_key, dims, cuts, -0.22, 0.18) * drawn
    return jnp.clip(drawn, min=-bound, max=bound).astype(kind)


def setup_inputs(seed: int = 0) -> dict:
    keys = jax.random.split(jax.random.key(seed), 12)
    observations = draw_observations(jax.random.fold_in(keys[11], 71), 0)
    counts = draw_counts(jax.random.fold_in(keys[11], 71), 0)
    visible = touch_ends((jax.random.randint(keys[2], (REGIONS, REGIONS), 0, 2) < 1).astype(jnp.int32), jax.random.fold_in(keys[2], 1), 0, 1)
    latents = gaussian(keys[3], (REGIONS, LR, D), 1.0, 6.0, ((0, 8),))
    lat_gain = jnp.clip(1.0 + 0.1 * jax.random.normal(keys[4], (D,), jnp.float32), 0.5, 1.5)
    mlp_gain = jnp.clip(1.0 + 0.1 * jax.random.normal(keys[5], (D,), jnp.float32), 0.5, 1.5)
    w_query = gaussian(keys[6], (D, D), D ** -0.5, 0.25)
    w_keyval = gaussian(keys[7], (D, 2 * D), D ** -0.5, 0.25)
    w_out = gaussian(keys[8], (D, D), D ** -0.5, 0.25)
    w_up = gaussian(keys[9], (D, HID), D ** -0.5, 0.25, ((1, 4),))
    w_down = gaussian(keys[10], (HID, D), HID ** -0.5, 0.125, ((0, 4),))
    return {"observations": observations, "counts": counts, "visible": visible, "latents": latents, "lat_gain": lat_gain, "mlp_gain": mlp_gain, "w_query": w_query, "w_keyval": w_keyval, "w_out": w_out, "w_up": w_up, "w_down": w_down}


NEG = -1e+30

def layer_norm(values, gain):
    average = lax.optimization_barrier(jnp.mean(values, axis=-1, keepdims=True))
    centered = values - average
    variance = lax.optimization_barrier(jnp.mean(centered * centered, axis=-1, keepdims=True))
    return centered * lax.rsqrt(variance + 1e-05) * gain

def expand(factor, model_width):
    return jnp.repeat(factor, model_width // factor.shape[-1], axis=-1)

def combine(first, second):
    first_num, first_den, first_peak = first
    second_num, second_den, second_peak = second
    highest = jnp.maximum(first_peak, second_peak)
    first_scale = jnp.exp(first_peak - highest)
    second_scale = jnp.exp(second_peak - highest)
    numerator = first_num * expand(first_scale, first_num.shape[-1]) + second_num * expand(second_scale, second_num.shape[-1])
    return (numerator, first_den * first_scale + second_den * second_scale, highest)

def partials(query_rows, key_rows, value_rows, allowed):
    row_count = query_rows.shape[0]
    key_count = key_rows.shape[0]
    query_heads = query_rows.astype(jnp.float32).reshape(row_count, H, DH)
    key_heads = key_rows.astype(jnp.float32).reshape(key_count, H, DH)
    value_heads = value_rows.astype(jnp.float32).reshape(key_count, H, DH)
    scores = jnp.einsum('qhd,khd->hqk', query_heads, key_heads) * DH ** (-0.5)
    scores = jnp.where(allowed[None], scores, NEG)
    peaks = lax.optimization_barrier(jnp.max(scores, axis=-1))
    weights = jnp.where(allowed[None], jnp.exp(scores - peaks[..., None]), 0.0)
    denominator = lax.optimization_barrier(jnp.sum(weights, axis=-1))
    rounded = weights.astype(jnp.bfloat16).astype(jnp.float32)
    numerator = jnp.einsum('hqk,khd->qhd', rounded, value_heads).reshape(row_count, H * DH)
    return (numerator, denominator.T, peaks.T)

def reference(observations, counts, visible, latents, lat_gain, mlp_gain, w_query, w_keyval, w_out, w_up, w_down):
    obs_rows = CAP * BLK

    def project(blocks):
        flat = blocks.reshape(SLOTS * obs_rows, D)
        return jnp.dot(flat, w_keyval, preferred_element_type=jnp.float32).astype(jnp.bfloat16).reshape(SLOTS, obs_rows, 2 * D)
    keyval = lax.map(project, observations)
    latent_rows = latents.astype(jnp.float32)
    normed = layer_norm(latent_rows, lat_gain).astype(jnp.bfloat16).reshape(REGIONS * LR, D)
    queries = jnp.dot(normed, w_query, preferred_element_type=jnp.float32).astype(jnp.bfloat16).reshape(REGIONS, LR, D)
    live_rows = jnp.arange(obs_rows, dtype=jnp.int32)[None, None, :] < counts[:, :, None] * BLK

    def per_latent(region_id):
        region_queries = queries[region_id]

        def step(carried, source_id):
            sees_source = (visible[region_id, source_id] > 0) | (region_id == source_id)

            def compute(unused):

                def per_slot(slot_id):
                    block = keyval[source_id, slot_id]
                    allowed = jnp.broadcast_to(live_rows[source_id, slot_id][None, :], (LR, obs_rows))
                    return partials(region_queries, block[:, :D], block[:, D:], allowed)
                nums, dens, peaks = lax.map(per_slot, jnp.arange(SLOTS, dtype=jnp.int32))
                result = (nums[0], dens[0], peaks[0])
                for slot_id in range(1, SLOTS):
                    result = combine(result, (nums[slot_id], dens[slot_id], peaks[slot_id]))
                return result

            def skipped(unused):
                return (jnp.zeros((LR, D), jnp.float32), jnp.zeros((LR, H), jnp.float32), jnp.full((LR, H), NEG, jnp.float32))
            piece_set = lax.cond(sees_source, compute, skipped, None)
            return (combine(carried, piece_set), None)
        initial = (jnp.zeros((LR, D), jnp.float32), jnp.zeros((LR, H), jnp.float32), jnp.full((LR, H), NEG, jnp.float32))
        final, unused = lax.scan(step, initial, jnp.arange(REGIONS, dtype=jnp.int32))
        return final[0] / expand(final[1], D)
    attended = lax.map(per_latent, jnp.arange(REGIONS, dtype=jnp.int32)).astype(jnp.bfloat16).reshape(REGIONS * LR, D)
    residual = latent_rows.reshape(REGIONS * LR, D) + jnp.dot(attended, w_out, preferred_element_type=jnp.float32)
    normed2 = layer_norm(residual, mlp_gain).astype(jnp.bfloat16)
    hidden = jax.nn.gelu(jnp.dot(normed2, w_up, preferred_element_type=jnp.float32), approximate=True).astype(jnp.bfloat16)
    encoded = residual + jnp.dot(hidden, w_down, preferred_element_type=jnp.float32)
    return encoded.astype(jnp.bfloat16).reshape(REGIONS, LR, D)
```

```python
import functools

import jax
import jax.numpy as jnp
from jax import lax
from jax.experimental import pallas as pl
from jax.experimental.pallas import tpu as pltpu
from jax.sharding import PartitionSpec as P

H = 8
BLK = 256
NEG = -1e30
TILE = 8
LANES = 128
F32 = jnp.float32
BF16 = jnp.bfloat16
MESH = pl.DeviceIdType.MESH


def layer_norm(values, gain):
    average = jnp.mean(values, axis=-1, keepdims=True)
    centered = values - average
    variance = jnp.mean(centered * centered, axis=-1, keepdims=True)
    return centered * lax.rsqrt(variance + 1e-05) * gain


def columns_of(table, first, heads, lane, head_size):
    spread = jnp.broadcast_to(table[:, first : first + 1], lane.shape)
    for h in range(1, heads):
        column = table[:, first + h : first + h + 1]
        spread = jnp.where(lane >= h * head_size, column, spread)
    return spread


def turned(tiles):
    short = -len(tiles) * TILE % LANES
    if short:
        tiles = tiles + [jnp.zeros((short, tiles[0].shape[1]), F32)]
    return jnp.concatenate(tiles, axis=0).T


def kernel(
    R, T, chunk, q_block, k_block,
    counts, visible, lat, lat_gain, mlp_gain,
    obs_h, wkv_h, wq_h, wout_h, wup_h, wdn_h,
    out,
    obs, wkv, wq, wout, wup, wdn,
    lat_all, keys, values, queries, scores,
    snum, saux, gnum, gaux,
    snum2, saux2, gnum2, gaux2,
    att_own, att_all, part_own, part_all,
    load_sem, obs_sem, lat_s, lat_r,
    n1_s, n1_r, a1_s, a1_r, n2_s, n2_r, a2_s, a2_r,
    att_s, att_r, part_s, part_r,
):
    me = lax.axis_index("region")
    t = lax.axis_index("tm")
    N, D = obs.shape
    LR = lat.shape[1]
    rows = R * LR
    DH = D // H
    G = D // T
    HG = G // DH

    def region_peer(d):
        return lax.rem(me + d, R)

    def tm_peer(d):
        return lax.rem(t + d, T)

    loads = [
        pltpu.make_async_copy(src, dst, load_sem.at[i])
        for i, (src, dst) in enumerate(
            [(wkv_h, wkv), (wq_h, wq), (wout_h, wout), (wup_h, wup), (wdn_h, wdn)]
        )
    ]

    def obs_load(c):
        at = pl.ds(pl.multiple_of(c * chunk, chunk), chunk)
        return pltpu.make_async_copy(obs_h.at[0, 0, at, :], obs.at[at, :], obs_sem.at[c])

    loads[0].start()
    for c in range(N // chunk):
        obs_load(c).start()
    for load in loads[1:]:
        load.start()

    barrier = pltpu.get_barrier_semaphore()
    for d in range(1, R):
        pl.semaphore_signal(barrier, inc=1, device_id=(region_peer(d), t), device_id_type=MESH)
    for d in range(1, T):
        pl.semaphore_signal(barrier, inc=1, device_id=(me, tm_peer(d)), device_id_type=MESH)
    pl.semaphore_wait(barrier, R + T - 2)

    def lat_copy(d):
        return pltpu.make_async_remote_copy(
            lat.at[0], lat_all.at[me], lat_s.at[d], lat_r.at[d],
            device_id=(region_peer(d), t), device_id_type=MESH,
        )

    for d in range(1, R):
        lat_copy(d).start()
    lat_all[me] = lat[0]

    loads[0].wait()

    def project(c, carry):
        obs_load(c).wait()
        at = pl.ds(pl.multiple_of(c * chunk, chunk), chunk)
        kv = jnp.dot(obs[at, :], wkv[...], preferred_element_type=F32).astype(BF16)
        for g in range(T):
            keys[g, at, :] = kv[:, g * G : (g + 1) * G]
            values[g, at, :] = kv[:, D + g * G : D + (g + 1) * G]
        return carry

    lax.fori_loop(0, N // chunk, project, 0)

    for load in loads[1:]:
        load.wait()
    for d in range(1, R):
        lat_copy(d).wait_recv()
    normed = layer_norm(lat_all[...].astype(F32).reshape(rows, D), lat_gain[...]).astype(BF16)
    every = jnp.dot(normed, wq[...], preferred_element_type=F32).astype(BF16).astype(F32)
    every = (every * DH ** (-0.5)).astype(BF16)
    for g in range(T):
        queries[g] = every[:, g * G : (g + 1) * G]

    live_rows = counts[0, 0] * BLK
    lane = lax.broadcasted_iota(jnp.int32, (q_block, G), 1)
    aux_lane = lax.broadcasted_iota(jnp.int32, (q_block, LANES), 1)
    head_mask = [
        ((lane >= h * DH) & (lane < (h + 1) * DH)).astype(F32) for h in range(HG)
    ]
    k_lane = lax.broadcasted_iota(jnp.int32, (1, k_block), 1)

    def num_copy(j):
        return pltpu.make_async_remote_copy(
            snum.at[j], gnum.at[j], n1_s.at[j], n1_r.at[j],
            device_id=(me, tm_peer(j + 1)), device_id_type=MESH,
        )

    def aux_copy(j):
        return pltpu.make_async_remote_copy(
            saux.at[j], gaux.at[j], a1_s.at[j], a1_r.at[j],
            device_id=(me, tm_peer(j + 1)), device_id_type=MESH,
        )

    def lanes_reduced(x, op):
        total = x[:, :LANES]
        for i in range(1, k_block // LANES):
            total = op(total, x[:, i * LANES : (i + 1) * LANES])
        return total

    def attend(j, carry):
        g = tm_peer(j + 1)
        for b in range(rows // q_block):
            at = pl.ds(b * q_block, q_block)
            asked = queries[g, at, :].astype(F32)
            asked = jnp.concatenate([asked * mask for mask in head_mask], axis=0).astype(BF16)
            top = None
            for i in range(N // k_block):
                s = lax.dot_general(
                    asked, keys[g, pl.ds(i * k_block, k_block), :],
                    (((1,), (1,)), ((), ())), preferred_element_type=F32,
                )
                s = s + jnp.where(k_lane + i * k_block < live_rows, 0.0, NEG)
                scores[i] = s
                most = lanes_reduced(s, jnp.maximum)
                top = most if top is None else jnp.maximum(top, most)
            peak = jnp.max(top, axis=-1, keepdims=True)
            den = None
            acc = None
            for i in range(N // k_block):
                w = jnp.exp(scores[i] - peak)
                part = lanes_reduced(w, jnp.add)
                den = part if den is None else den + part
                num = jnp.dot(
                    w.astype(BF16), values[g, pl.ds(i * k_block, k_block), :],
                    preferred_element_type=F32,
                )
                acc = num if acc is None else acc + num
            den = jnp.sum(den, axis=-1, keepdims=True)
            num = acc[:q_block]
            aux = jnp.zeros((q_block, LANES), F32)
            for h in range(HG):
                rows_h = slice(h * q_block, (h + 1) * q_block)
                if h:
                    num = jnp.where(lane >= h * DH, acc[rows_h], num)
                aux = jnp.where(aux_lane == h, peak[rows_h], aux)
                aux = jnp.where(aux_lane == TILE + h, den[rows_h], aux)
            snum[j, at, :] = num.astype(BF16)
            saux[j, :, at] = aux.T[: 2 * TILE]

        @pl.when(j < T - 1)
        def _():
            num_copy(j).start()
            aux_copy(j).start()

        return carry

    lax.fori_loop(0, T, attend, 0)

    for j in range(T - 1):
        aux_copy(j).wait_recv()
    parts = [gaux[j] for j in range(T - 1)] + [saux[T - 1]]
    peaks = [part[:TILE] for part in parts]
    dens = [part[TILE:] for part in parts]
    highest = functools.reduce(jnp.maximum, peaks)
    factors = [jnp.exp(peak - highest) for peak in peaks]
    den = functools.reduce(jnp.add, [f * x for f, x in zip(factors, dens)])
    table = turned(factors)
    lane_all = lax.broadcasted_iota(jnp.int32, (rows, G), 1)
    num = snum[T - 1].astype(F32) * columns_of(table, (T - 1) * TILE, HG, lane_all, DH)
    for j in range(T - 1):
        num_copy(j).wait_recv()
        num += gnum[j].astype(F32) * columns_of(table, j * TILE, HG, lane_all, DH)
    snum2[...] = num.astype(BF16).reshape(R, LR, G)
    for r in range(R):
        seen = ((visible[r, me] > 0) | (me == r)).astype(F32)
        shift = (rows - r * LR) % rows
        peak_r = (pltpu.roll(highest, shift, 1) if shift else highest)[:, :LANES]
        den_r = (pltpu.roll(den, shift, 1) if shift else den)[:, :LANES]
        saux2[r, :TILE, :] = peak_r * seen + (1.0 - seen) * NEG
        saux2[r, TILE:, :] = den_r

    def num2_copy(d):
        return pltpu.make_async_remote_copy(
            snum2.at[region_peer(d)], gnum2.at[d], n2_s.at[d], n2_r.at[d],
            device_id=(region_peer(d), t), device_id_type=MESH,
        )

    def aux2_copy(d):
        return pltpu.make_async_remote_copy(
            saux2.at[region_peer(d)], gaux2.at[d], a2_s.at[d], a2_r.at[d],
            device_id=(region_peer(d), t), device_id_type=MESH,
        )

    for d in range(1, R):
        num2_copy(d).start()
        aux2_copy(d).start()
    for d in range(1, R):
        aux2_copy(d).wait_recv()
    parts = [saux2[me]] + [gaux2[d] for d in range(1, R)]
    peaks = [part[:TILE] for part in parts]
    highest = functools.reduce(jnp.maximum, peaks)
    factors = [jnp.exp(peak - highest) for peak in peaks]
    den = functools.reduce(jnp.add, [f * x[TILE:] for f, x in zip(factors, parts)])
    table = turned(factors + [den])[:LR]
    lane_own = lax.broadcasted_iota(jnp.int32, (LR, G), 1)
    num = snum2[me].astype(F32) * columns_of(table, 0, HG, lane_own, DH)
    for d in range(1, R):
        num2_copy(d).wait_recv()
        num += gnum2[d].astype(F32) * columns_of(table, d * TILE, HG, lane_own, DH)
    attended = (num / columns_of(table, R * TILE, HG, lane_own, DH)).astype(BF16)
    att_own[...] = attended
    att_all[t] = attended

    def att_copy(d):
        return pltpu.make_async_remote_copy(
            att_own, att_all.at[t], att_s.at[d], att_r.at[d],
            device_id=(me, tm_peer(d)), device_id_type=MESH,
        )

    for d in range(1, T):
        att_copy(d).start()
    for d in range(1, T):
        att_copy(d).wait_recv()

    residual = lat[0].astype(F32)
    residual += functools.reduce(
        jnp.add,
        [
            jnp.dot(att_all[g], wout[g * G : (g + 1) * G, :], preferred_element_type=F32)
            for g in range(T)
        ],
    )
    normed2 = layer_norm(residual, mlp_gain[...]).astype(BF16)
    hidden = jax.nn.gelu(
        jnp.dot(normed2, wup[...], preferred_element_type=F32), approximate=True
    ).astype(BF16)
    part = jnp.dot(hidden, wdn[...], preferred_element_type=F32).astype(BF16)
    part_own[...] = part
    part_all[t] = part

    def part_copy(d):
        return pltpu.make_async_remote_copy(
            part_own, part_all.at[t], part_s.at[d], part_r.at[d],
            device_id=(me, tm_peer(d)), device_id_type=MESH,
        )

    for d in range(1, T):
        part_copy(d).start()
    for d in range(1, T):
        part_copy(d).wait_recv()
    total = functools.reduce(jnp.add, [part_all[g].astype(F32) for g in range(T)])
    out[0] = (residual + total).astype(BF16)

    for d in range(1, R):
        lat_copy(d).wait_send()
        num2_copy(d).wait_send()
        aux2_copy(d).wait_send()
    for d in range(1, T):
        num_copy(d - 1).wait_send()
        aux_copy(d - 1).wait_send()
        att_copy(d).wait_send()
        part_copy(d).wait_send()


def on_device(
    R, T, observations, counts, visible, latents, lat_gain, mlp_gain,
    w_query, w_keyval, w_out, w_up, w_down,
):
    N, D = observations.shape[2:]
    LR = latents.shape[1]
    rows = R * LR
    G = D // T
    HG = G // (D // H)
    chunk = min(N, 512)
    q_block = min(rows, 256)
    k_block = min(N, 256)
    vmem = pl.BlockSpec(memory_space=pltpu.VMEM)
    smem = pl.BlockSpec(memory_space=pltpu.SMEM)
    any_space = pl.BlockSpec(memory_space=pl.ANY)
    dma = pltpu.SemaphoreType.DMA
    return pl.pallas_call(
        functools.partial(kernel, R, T, chunk, q_block, k_block),
        out_shape=jax.ShapeDtypeStruct((1, LR, D), BF16),
        in_specs=[smem, smem, vmem, vmem, vmem] + [any_space] * 6,
        out_specs=vmem,
        scratch_shapes=[
            pltpu.VMEM((N, D), BF16),
            pltpu.VMEM(w_keyval.shape, BF16),
            pltpu.VMEM(w_query.shape, BF16),
            pltpu.VMEM(w_out.shape, BF16),
            pltpu.VMEM(w_up.shape, BF16),
            pltpu.VMEM(w_down.shape, BF16),
            pltpu.VMEM((R, LR, D), BF16),
            pltpu.VMEM((T, N, G), BF16),
            pltpu.VMEM((T, N, G), BF16),
            pltpu.VMEM((T, rows, G), BF16),
            pltpu.VMEM((N // k_block, HG * q_block, k_block), F32),
            pltpu.VMEM((T, rows, G), BF16),
            pltpu.VMEM((T, 2 * TILE, rows), F32),
            pltpu.VMEM((T, rows, G), BF16),
            pltpu.VMEM((T, 2 * TILE, rows), F32),
            pltpu.VMEM((R, LR, G), BF16),
            pltpu.VMEM((R, 2 * TILE, LANES), F32),
            pltpu.VMEM((R, LR, G), BF16),
            pltpu.VMEM((R, 2 * TILE, LANES), F32),
            pltpu.VMEM((LR, G), BF16),
            pltpu.VMEM((T, LR, G), BF16),
            pltpu.VMEM((LR, D), BF16),
            pltpu.VMEM((T, LR, D), BF16),
            dma((5,)), dma((N // chunk,)), dma((R,)), dma((R,)),
            dma((T,)), dma((T,)), dma((T,)), dma((T,)),
            dma((R,)), dma((R,)), dma((R,)), dma((R,)),
            dma((T,)), dma((T,)), dma((T,)), dma((T,)),
        ],
        compiler_params=pltpu.CompilerParams(collective_id=0, has_side_effects=True),
    )(
        counts, visible, latents, lat_gain.reshape(1, D), mlp_gain.reshape(1, D),
        observations, w_keyval, w_query, w_out, w_up, w_down,
    )


def solution(mesh):
    placed = (
        P("region", "tm", None, None),
        P("region", "tm"),
        P(),
        P("region", None, None),
        P(),
        P(),
        P(),
        P(),
        P(),
        P(None, "tm"),
        P("tm", None),
    )
    return jax.shard_map(
        functools.partial(on_device, mesh.shape["region"], mesh.shape["tm"]),
        mesh=mesh, in_specs=placed, out_specs=P("region", None, None), check_vma=False,
    )
```

```python
import functools

import jax
import jax.numpy as jnp
from jax import lax
from jax.experimental import pallas as pl
from jax.experimental.pallas import tpu as pltpu
from jax.sharding import PartitionSpec as P

H = 8
BLK = 256
NEG = -1e30
TILE = 8
HALF = TILE // 2
LANES = 128
F32 = jnp.float32
BF16 = jnp.bfloat16
MESH = pl.DeviceIdType.MESH


def layer_norm(values, gain):
    average = jnp.mean(values, axis=-1, keepdims=True)
    centered = values - average
    variance = jnp.mean(centered * centered, axis=-1, keepdims=True)
    return centered * lax.rsqrt(variance + 1e-05) * gain


def columns_of(table, first, heads, lane, head_size):
    spread = jnp.broadcast_to(table[:, first : first + 1], lane.shape)
    for h in range(1, heads):
        column = table[:, first + h : first + h + 1]
        spread = jnp.where(lane >= h * head_size, column, spread)
    return spread


def joined(parts):
    highest = functools.reduce(jnp.maximum, parts)
    factors = [jnp.exp(part - highest) for part in parts]
    den = functools.reduce(
        jnp.add, [pltpu.roll(f, HALF, 0) * part for f, part in zip(factors, parts)]
    )
    return highest, factors, den


def turned(tiles):
    short = -len(tiles) * TILE % LANES
    if short:
        tiles = tiles + [jnp.zeros((short, tiles[0].shape[1]), F32)]
    return jnp.concatenate(tiles, axis=0).T


def kernel(
    R, T, chunk, q_block, row_slice,
    counts, visible, lat, lat_gain, mlp_gain,
    obs_h, wkv_h, wq_h, wout_h, wup_h, wdn_h,
    out,
    obs, wkv, wq, wout, wup, wdn,
    lat_all, keys, values, queries, scores, weights,
    snum, saux, gnum, gaux,
    snum2, saux2, gnum2, gaux2,
    att_own, att_all, part_own, part_all,
    load_sem, obs_sem, lat_s, lat_r, mate_s, mate_r,
    n1_s, n1_r, a1_s, a1_r, n2_s, n2_r, a2_s, a2_r,
    att_s, att_r, part_s, part_r,
):
    me = lax.axis_index("region")
    t = lax.axis_index("tm")
    N, D = obs.shape
    LR = lat.shape[1]
    rows = R * LR
    DH = D // H
    G = D // T
    HG = G // DH

    def region_peer(d):
        return lax.rem(me + d, R)

    def tm_peer(d):
        return lax.rem(t + d, T)

    loads = [
        pltpu.make_async_copy(src, dst, load_sem.at[i])
        for i, (src, dst) in enumerate(
            [(wkv_h, wkv), (wq_h, wq), (wout_h, wout), (wup_h, wup), (wdn_h, wdn)]
        )
    ]

    def obs_load(c):
        at = pl.ds(pl.multiple_of(c * chunk, chunk), chunk)
        return pltpu.make_async_copy(obs_h.at[0, 0, at, :], obs.at[at, :], obs_sem.at[c])

    loads[0].start()
    for c in range(N // chunk):
        obs_load(c).start()
    for load in loads[1:]:
        load.start()

    barrier = pltpu.get_barrier_semaphore()
    for d in range(1, R):
        pl.semaphore_signal(barrier, inc=1, device_id=(region_peer(d), t), device_id_type=MESH)
    for d in range(1, T):
        pl.semaphore_signal(barrier, inc=1, device_id=(me, tm_peer(d)), device_id_type=MESH)
    pl.semaphore_wait(barrier, R + T - 2)

    halves = 2 if T % 2 == 0 else 1
    half = LR // halves
    mate = t + 1 - 2 * lax.rem(t, 2)
    mine = pl.ds(pl.multiple_of(lax.rem(t, halves) * half, half), half)

    def lat_copy(d):
        return pltpu.make_async_remote_copy(
            lat.at[0, mine, :], lat_all.at[me, mine, :], lat_s.at[d], lat_r.at[d],
            device_id=(region_peer(d), t), device_id_type=MESH,
        )

    def mate_copy(d):
        source = region_peer(R - d)
        return pltpu.make_async_remote_copy(
            lat_all.at[source, mine, :], lat_all.at[source, mine, :], mate_s.at[d], mate_r.at[d],
            device_id=(me, mate), device_id_type=MESH,
        )

    for d in range(1, R):
        lat_copy(d).start()
    lat_all[me] = lat[0]

    loads[0].wait()

    def project(c, carry):
        obs_load(c).wait()
        at = pl.ds(pl.multiple_of(c * chunk, chunk), chunk)
        kv = jnp.dot(obs[at, :], wkv[...], preferred_element_type=F32).astype(BF16)
        for g in range(T):
            keys[g, at, :] = kv[:, g * G : (g + 1) * G]
            values[g, at, :] = kv[:, D + g * G : D + (g + 1) * G]
        return carry

    lax.fori_loop(0, N // chunk, project, 0)

    loads[1].wait()
    for d in range(1, R):
        lat_copy(d).wait_recv()
        if halves == 2:
            mate_copy(d).start()
    if halves == 2:
        for d in range(1, R):
            mate_copy(d).wait_recv()
    normed = layer_norm(lat_all[...].astype(F32).reshape(rows, D), lat_gain[...]).astype(BF16)
    every = jnp.dot(normed, wq[...], preferred_element_type=F32).astype(BF16).astype(F32)
    every = (every * DH ** (-0.5)).astype(BF16)
    for g in range(T):
        queries[g] = every[:, g * G : (g + 1) * G]

    live_rows = counts[0, 0] * BLK
    lane = lax.broadcasted_iota(jnp.int32, (q_block, G), 1)
    aux_lane = lax.broadcasted_iota(jnp.int32, (q_block, LANES), 1)
    head_mask = [
        ((lane >= h * DH) & (lane < (h + 1) * DH)).astype(F32) for h in range(HG)
    ]
    live = lax.broadcasted_iota(jnp.int32, (1, N), 1) < live_rows

    def num_copy(j):
        return pltpu.make_async_remote_copy(
            snum.at[j], gnum.at[j], n1_s.at[j], n1_r.at[j],
            device_id=(me, tm_peer(j + 1)), device_id_type=MESH,
        )

    def aux_copy(j):
        return pltpu.make_async_remote_copy(
            saux.at[j], gaux.at[j], a1_s.at[j], a1_r.at[j],
            device_id=(me, tm_peer(j + 1)), device_id_type=MESH,
        )

    def lanes_reduced(x, op):
        return functools.reduce(op, [x[:, i : i + LANES] for i in range(0, N, LANES)])

    def attend(j, carry):
        g = tm_peer(j + 1)
        bias = jnp.where(live, 0.0, NEG)
        for b in range(rows // q_block):
            at = pl.ds(b * q_block, q_block)
            asked = queries[g, at, :].astype(F32)
            asked = jnp.concatenate([asked * mask for mask in head_mask], axis=0).astype(BF16)
            scores[b] = bias + lax.dot_general(
                asked, keys[g], (((1,), (1,)), ((), ())), preferred_element_type=F32
            )
        for b in range(rows // q_block):
            at = pl.ds(b * q_block, q_block)
            peaks = []
            dens = []
            for r in range(0, HG * q_block, row_slice):
                s = scores[b, r : r + row_slice, :]
                peak = jnp.max(lanes_reduced(s, jnp.maximum), axis=-1, keepdims=True)
                w = jnp.exp(s - peak)
                dens.append(jnp.sum(lanes_reduced(w, jnp.add), axis=-1, keepdims=True))
                peaks.append(peak)
                weights[b, r : r + row_slice, :] = w.astype(BF16)
            acc = jnp.dot(weights[b], values[g], preferred_element_type=F32)
            peak = jnp.concatenate(peaks, axis=0)
            den = jnp.concatenate(dens, axis=0)
            num = acc[:q_block]
            aux = jnp.zeros((q_block, LANES), F32)
            for h in range(HG):
                rows_h = slice(h * q_block, (h + 1) * q_block)
                if h:
                    num = jnp.where(lane >= h * DH, acc[rows_h], num)
                aux = jnp.where(aux_lane == h, peak[rows_h], aux)
                aux = jnp.where(aux_lane == HALF + h, den[rows_h], aux)
            snum[j, at, :] = num.astype(BF16)
            saux[j, :, at] = aux.T[:TILE]

        @pl.when(j < T - 1)
        def _():
            num_copy(j).start()
            aux_copy(j).start()

        return carry

    lax.fori_loop(0, T, attend, 0)

    for j in range(T - 1):
        aux_copy(j).wait_recv()
    parts = [gaux[j] for j in range(T - 1)] + [saux[T - 1]]
    highest, factors, den = joined(parts)
    table = turned(factors)
    lane_all = lax.broadcasted_iota(jnp.int32, (rows, G), 1)
    num = snum[T - 1].astype(F32) * columns_of(table, (T - 1) * TILE, HG, lane_all, DH)
    for j in range(T - 1):
        num_copy(j).wait_recv()
        num += gnum[j].astype(F32) * columns_of(table, j * TILE, HG, lane_all, DH)
    snum2[...] = num.astype(BF16).reshape(R, LR, G)
    merged = jnp.where(lax.broadcasted_iota(jnp.int32, den.shape, 0) < HALF, highest, den)
    is_peak = lax.broadcasted_iota(jnp.int32, (TILE, LANES), 0) < HALF
    for r in range(R):
        seen = ((visible[r, me] > 0) | (me == r)).astype(F32)
        shift = (rows - r * LR) % rows
        tile = (pltpu.roll(merged, shift, 1) if shift else merged)[:, :LANES]
        saux2[r] = jnp.where(is_peak, tile * seen + (1.0 - seen) * NEG, tile)

    def num2_copy(d):
        return pltpu.make_async_remote_copy(
            snum2.at[region_peer(d)], gnum2.at[d], n2_s.at[d], n2_r.at[d],
            device_id=(region_peer(d), t), device_id_type=MESH,
        )

    def aux2_copy(d):
        return pltpu.make_async_remote_copy(
            saux2.at[region_peer(d)], gaux2.at[d], a2_s.at[d], a2_r.at[d],
            device_id=(region_peer(d), t), device_id_type=MESH,
        )

    for d in range(1, R):
        num2_copy(d).start()
        aux2_copy(d).start()
    for d in range(1, R):
        aux2_copy(d).wait_recv()
    parts = [saux2[me]] + [gaux2[d] for d in range(1, R)]
    highest, factors, den = joined(parts)
    table = turned(factors + [den])[:LR]
    lane_own = lax.broadcasted_iota(jnp.int32, (LR, G), 1)
    num = snum2[me].astype(F32) * columns_of(table, 0, HG, lane_own, DH)
    for d in range(1, R):
        num2_copy(d).wait_recv()
        num += gnum2[d].astype(F32) * columns_of(table, d * TILE, HG, lane_own, DH)
    attended = (num / columns_of(table, R * TILE + HALF, HG, lane_own, DH)).astype(BF16)
    att_own[...] = attended
    att_all[t] = attended

    def att_copy(d):
        return pltpu.make_async_remote_copy(
            att_own, att_all.at[t], att_s.at[d], att_r.at[d],
            device_id=(me, tm_peer(d)), device_id_type=MESH,
        )

    for d in range(1, T):
        att_copy(d).start()
    for d in range(1, T):
        att_copy(d).wait_recv()

    for load in loads[2:]:
        load.wait()

    residual = lat[0].astype(F32)
    residual += functools.reduce(
        jnp.add,
        [
            jnp.dot(att_all[g], wout[g * G : (g + 1) * G, :], preferred_element_type=F32)
            for g in range(T)
        ],
    )
    normed2 = layer_norm(residual, mlp_gain[...]).astype(BF16)
    hidden = jax.nn.gelu(
        jnp.dot(normed2, wup[...], preferred_element_type=F32), approximate=True
    ).astype(BF16)
    part = jnp.dot(hidden, wdn[...], preferred_element_type=F32).astype(BF16)
    part_own[...] = part
    part_all[t] = part

    def part_copy(d):
        return pltpu.make_async_remote_copy(
            part_own, part_all.at[t], part_s.at[d], part_r.at[d],
            device_id=(me, tm_peer(d)), device_id_type=MESH,
        )

    for d in range(1, T):
        part_copy(d).start()
    for d in range(1, T):
        part_copy(d).wait_recv()
    total = functools.reduce(jnp.add, [part_all[g].astype(F32) for g in range(T)])
    out[0] = (residual + total).astype(BF16)

    for d in range(1, R):
        lat_copy(d).wait_send()
        if halves == 2:
            mate_copy(d).wait_send()
        num2_copy(d).wait_send()
        aux2_copy(d).wait_send()
    for d in range(1, T):
        num_copy(d - 1).wait_send()
        aux_copy(d - 1).wait_send()
        att_copy(d).wait_send()
        part_copy(d).wait_send()


def on_device(
    R, T, observations, counts, visible, latents, lat_gain, mlp_gain,
    w_query, w_keyval, w_out, w_up, w_down,
):
    N, D = observations.shape[2:]
    LR = latents.shape[1]
    rows = R * LR
    G = D // T
    HG = G // (D // H)
    chunk = min(N, 512)
    q_block = min(rows, 128)
    row_slice = min(q_block, 16)
    vmem = pl.BlockSpec(memory_space=pltpu.VMEM)
    smem = pl.BlockSpec(memory_space=pltpu.SMEM)
    any_space = pl.BlockSpec(memory_space=pl.ANY)
    dma = pltpu.SemaphoreType.DMA
    return pl.pallas_call(
        functools.partial(kernel, R, T, chunk, q_block, row_slice),
        out_shape=jax.ShapeDtypeStruct((1, LR, D), BF16),
        in_specs=[smem, smem, vmem, vmem, vmem] + [any_space] * 6,
        out_specs=vmem,
        scratch_shapes=[
            pltpu.VMEM((N, D), BF16),
            pltpu.VMEM(w_keyval.shape, BF16),
            pltpu.VMEM(w_query.shape, BF16),
            pltpu.VMEM(w_out.shape, BF16),
            pltpu.VMEM(w_up.shape, BF16),
            pltpu.VMEM(w_down.shape, BF16),
            pltpu.VMEM((R, LR, D), BF16),
            pltpu.VMEM((T, N, G), BF16),
            pltpu.VMEM((T, N, G), BF16),
            pltpu.VMEM((T, rows, G), BF16),
            pltpu.VMEM((rows // q_block, HG * q_block, N), F32),
            pltpu.VMEM((rows // q_block, HG * q_block, N), BF16),
            pltpu.VMEM((T, rows, G), BF16),
            pltpu.VMEM((T, TILE, rows), F32),
            pltpu.VMEM((T, rows, G), BF16),
            pltpu.VMEM((T, TILE, rows), F32),
            pltpu.VMEM((R, LR, G), BF16),
            pltpu.VMEM((R, TILE, LANES), F32),
            pltpu.VMEM((R, LR, G), BF16),
            pltpu.VMEM((R, TILE, LANES), F32),
            pltpu.VMEM((LR, G), BF16),
            pltpu.VMEM((T, LR, G), BF16),
            pltpu.VMEM((LR, D), BF16),
            pltpu.VMEM((T, LR, D), BF16),
            dma((5,)), dma((N // chunk,)), dma((R,)), dma((R,)), dma((R,)), dma((R,)),
            dma((T,)), dma((T,)), dma((T,)), dma((T,)),
            dma((R,)), dma((R,)), dma((R,)), dma((R,)),
            dma((T,)), dma((T,)), dma((T,)), dma((T,)),
        ],
        compiler_params=pltpu.CompilerParams(collective_id=0, has_side_effects=True),
    )(
        counts, visible, latents, lat_gain.reshape(1, D), mlp_gain.reshape(1, D),
        observations, w_keyval, w_query, w_out, w_up, w_down,
    )


def solution(mesh):
    placed = (
        P("region", "tm", None, None),
        P("region", "tm"),
        P(),
        P("region", None, None),
        P(),
        P(),
        P(),
        P(),
        P(),
        P(None, "tm"),
        P("tm", None),
    )
    return jax.shard_map(
        functools.partial(on_device, mesh.shape["region"], mesh.shape["tm"]),
        mesh=mesh, in_specs=placed, out_specs=P("region", None, None), check_vma=False,
    )
```
